32 devices in a mesh: tok: 16 (over z, y, core), lay: 2 (over x).
Axes of the slice: x: 2, y: 2, z: 4, core: 2. Of those that a mesh axis runs over, the one named last changes fastest.
Arguments:
- first_acts: bfloat16 [2, 4096, 5120], P('lay', 'tok'), may hold values from -40 to 40
- second_acts: bfloat16 [2, 4096, 5120], P('lay', 'tok'), may hold values from -40 to 40
Outputs:
- whitening: float32 [2, 2, 40, 128, 128], P(None, 'lay')
- similarity: float32 [2, 2, 40], P('lay')
The draws below stay inside these ranges and needn't reach their ends.
All inputs are finite; a program needn't handle non-finite values.
Results may differ from the reference program's by a relative error of at most 0.0003.
Values may be sent and summed in bfloat16 or wider, within the bound.
A program may use at most 128 MiB of HBM per device.

```python
import math
import jax
import jax.numpy as jnp
from jax import lax

HEADS = 40
HEAD_DIM = 128
D = 5120
ITERS = 6
LAYERS = 2
TOKENS = 4096


def residual_layers(key):
    row_position = jnp.arange(TOKENS, dtype=jnp.float32) / TOKENS
    row_jitter = jax.random.uniform(jax.random.fold_in(key, 11), (TOKENS,), jnp.float32, -0.35, 0.35)
    row_scale = jnp.exp(math.log(3.0) * row_position + row_jitter)
    mixing = jnp.eye(HEAD_DIM, dtype=jnp.float32) + 0.8 / math.sqrt(HEAD_DIM) * jax.random.normal(jax.random.fold_in(key, 12), (HEADS, HEAD_DIM, HEAD_DIM), jnp.float32)
    stream = jnp.zeros((TOKENS, D), jnp.float32)
    first_list = []
    second_list = []
    for layer_idx in range(LAYERS):
        layer_key = jax.random.fold_in(key, 1000 + layer_idx)
        update = jax.random.normal(jax.random.fold_in(layer_key, 1), (TOKENS, D), jnp.float32)
        noise_part = jax.random.normal(jax.random.fold_in(layer_key, 3), (TOKENS, D), jnp.float32)
        chan_low = 0.3
        chan_high = 3.0
        stream = 0.8 * stream + 0.6 * update
        mixed_stream = jnp.einsum('thi,hij->thj', stream.reshape(TOKENS, HEADS, HEAD_DIM), mixing, precision=lax.Precision.HIGHEST).reshape(TOKENS, D)
        chan_first = jnp.exp(jax.random.uniform(jax.random.fold_in(layer_key, 4), (D,), jnp.float32, math.log(chan_low), math.log(chan_high)))
        chan_second = chan_first * jnp.exp(jax.random.uniform(jax.random.fold_in(layer_key, 5), (D,), jnp.float32, -0.35, 0.35))
        offset_first = 0.8 * jax.random.normal(jax.random.fold_in(layer_key, 6), (D,), jnp.float32)
        offset_second = offset_first + 0.3 * jax.random.normal(jax.random.fold_in(layer_key, 7), (D,), jnp.float32)
        first_layer = row_scale[:, None] * (chan_first * mixed_stream + offset_first)
        second_layer = row_scale[:, None] * (chan_second * (0.75 * mixed_stream + 0.66 * noise_part) + offset_second)
        first_list.append(jnp.clip(first_layer, -40.0, 40.0))
        second_list.append(jnp.clip(second_layer, -40.0, 40.0))
    return (jnp.stack(first_list), jnp.stack(second_list))


def draw_first_acts(key, part):
    return residual_layers(key)[0].astype(jnp.bfloat16)


def draw_second_acts(key, part):
    return residual_layers(key)[1].astype(jnp.bfloat16)


def setup_inputs(seed: int = 0) -> dict:
    arg_keys = jax.random.split(jax.random.key(seed), 3)
    return {
        "first_acts": draw_first_acts(jax.random.fold_in(arg_keys[2], 71), 0),
        "second_acts": draw_second_acts(jax.random.fold_in(arg_keys[2], 71), 0),
    }


ridge_weight = 0.05
top_precision = lax.Precision.HIGHEST

def newton_whiten(matrices):
    unit_matrix = jnp.eye(HEAD_DIM, dtype=jnp.float32)
    scale_norm = jnp.sqrt(lax.optimization_barrier(jnp.sum(matrices * matrices, axis=(-2, -1), keepdims=True)))
    square_iter = matrices / scale_norm
    inverse_iter = jnp.broadcast_to(unit_matrix, matrices.shape)
    for sweep_index in range(ITERS):
        factor_iter = 1.5 * unit_matrix - 0.5 * jnp.matmul(inverse_iter, square_iter, precision=top_precision)
        square_iter = jnp.matmul(square_iter, factor_iter, precision=top_precision)
        inverse_iter = jnp.matmul(factor_iter, inverse_iter, precision=top_precision)
    return inverse_iter / jnp.sqrt(scale_norm)

def covariance(gram_total, col_sums, token_total):
    unit_matrix = jnp.eye(HEAD_DIM, dtype=jnp.float32)
    column_mean = col_sums / token_total
    return gram_total / token_total - column_mean[..., :, None] * column_mean[..., None, :] + ridge_weight * unit_matrix

def head_view(act_block):
    return act_block.astype(jnp.float32).reshape(TOKENS, HEADS, HEAD_DIM)

def reference(first_acts, second_acts):
    gram_list = []
    sums_list = []
    for checkpoint in (first_acts, second_acts):
        for layer_idx in range(LAYERS):
            viewed = head_view(checkpoint[layer_idx])
            gram_list.append(jnp.einsum('thi,thj->hij', viewed, viewed, precision=top_precision))
            sums_list.append(lax.optimization_barrier(jnp.sum(viewed, axis=0)))
    gram_total = jnp.stack(gram_list).reshape(2, LAYERS, HEADS, HEAD_DIM, HEAD_DIM)
    col_sums = jnp.stack(sums_list).reshape(2, LAYERS, HEADS, HEAD_DIM)
    whitening = newton_whiten(covariance(gram_total, col_sums, TOKENS))
    column_mean = col_sums / TOKENS
    rows_out = []
    for first_idx in range(LAYERS):
        view_first = head_view(first_acts[first_idx])
        row_items = []
        for second_idx in range(LAYERS):
            view_second = head_view(second_acts[second_idx])
            cross_cov = jnp.einsum('thi,thj->hij', view_first, view_second, precision=top_precision) / TOKENS
            cross_cov = cross_cov - column_mean[0, first_idx][:, :, None] * column_mean[1, second_idx][:, None, :]
            left_product = jnp.matmul(whitening[0, first_idx], cross_cov, precision=top_precision)
            whitened = jnp.matmul(left_product, whitening[1, second_idx], precision=top_precision)
            row_items.append(lax.optimization_barrier(jnp.sum(whitened * whitened, axis=(-2, -1))) / HEAD_DIM)
        rows_out.append(jnp.stack(row_items))
    return (whitening, jnp.stack(rows_out))
```

```python
import functools

import jax
import jax.numpy as jnp
from jax import lax
from jax.experimental import pallas as pl
from jax.experimental.pallas import tpu as pltpu
from jax.sharding import PartitionSpec as P

HEADS = 40
HEAD_DIM = 128
ITERS = 6
PAD = 8

ridge_weight = 0.05
MESH = pl.DeviceIdType.MESH
HI = lax.Precision.HIGHEST


def dot_tt(a, b, precision=None):
    return lax.dot_general(
        a, b, (((0,), (0,)), ((), ())), preferred_element_type=jnp.float32, precision=precision
    )


def mm(a, b):
    return jnp.dot(a, b, preferred_element_type=jnp.float32, precision=HI)


def kernel(
    n, R, hp, token_total,
    x1, x2, out, simout,
    x2o, gp, gd, gy, gz, cp, cd, cy, cz, slab, wbuf, sbuf, yb, zb,
    x_s, x_r, gd_s, gd_r, gy_s, gy_r, gz_s, gz_r,
    cd_s, cd_r, cy_s, cy_r, cz_s, cz_r,
    p_s, p_r, q_s, q_r, az_s, az_r, ay_s, ay_r, ad_s, ad_r, ss_s, ss_r, o_s,
):
    me = lax.axis_index("tok")
    lay = lax.axis_index("lay")
    other = 1 - lay
    c = lax.rem(me, 2)
    y = lax.rem(me // 2, 2)
    z = me // 4
    rows = x1.shape[0]
    D = HEAD_DIM
    core_peer = z * 4 + y * 2 + (1 - c)
    y_peer = z * 4 + (1 - y) * 2 + c

    def z_peer(zt):
        return zt * 4 + y * 2 + c

    def rc(src, dst, s, r, tok, ly):
        return pltpu.make_async_remote_copy(
            src_ref=src, dst_ref=dst, send_sem=s, recv_sem=r,
            device_id=(tok, ly), device_id_type=MESH,
        )

    barrier = pltpu.get_barrier_semaphore()
    for k in range(1, n):
        pl.semaphore_signal(barrier, inc=1, device_id=(lax.rem(me + k, n), lay), device_id_type=MESH)
    pl.semaphore_signal(barrier, inc=1, device_id=(me, other), device_id_type=MESH)
    pl.semaphore_wait(barrier, n)

    zts = [lax.rem(z + 1 + i, R) for i in range(R)]
    sends = []

    padded = R * 2 * hp != HEADS
    width = x1.shape[1] // R if not padded else x1.shape[1]
    x_parts = []
    for i in range(R if not padded else 1):
        cols = pl.ds(pl.multiple_of(zts[i] * width, 128), width) if not padded else pl.ds(0, width)
        d = rc(x2.at[:, cols], x2o.at[:, cols], x_s.at[i], x_r.at[i], me, other)
        d.start()
        x_parts.append(d)
        sends.append(d)

    def head_cols(zt, yy, j):
        h = (zt * 2 + yy) * hp + j
        if padded:
            h = jnp.minimum(h, HEADS - 1)
        return pl.ds(pl.multiple_of(h * D, D), D)

    ones = jnp.ones((PAD, rows), jnp.bfloat16)

    g_d = []
    for i in range(R):
        zt = zts[i]

        def gram_body(j, carry, zt=zt):
            for yy in range(2):
                cols = head_cols(zt, yy, j)
                for k, ref in enumerate((x1, x2)):
                    v = ref[:, cols]
                    gp[k, zt, yy, j, :D, :] = dot_tt(v, v)
                    gp[k, zt, yy, j, D:, :] = jnp.dot(ones, v, preferred_element_type=jnp.float32)
            return carry

        lax.fori_loop(0, hp, gram_body, 0)
        d = rc(gp.at[1 - c, zt], gd.at[zt], gd_s.at[i], gd_r.at[i], core_peer, lay)
        d.start()
        g_d.append(d)
        sends.append(d)

    def y_phase(part, dbuf, ybuf, s, r, d_list):
        out_list = []
        for i in range(R):
            zt = zts[i]
            d_list[i].wait_recv()

            def add_body(j, carry, zt=zt):
                part[c, zt, 1 - y, j] = part[c, zt, 1 - y, j] + dbuf[zt, 1 - y, j]
                return carry

            lax.fori_loop(0, hp, add_body, 0)
            d = rc(part.at[c, zt, 1 - y], ybuf.at[zt], s.at[i], r.at[i], y_peer, lay)
            d.start()
            out_list.append(d)
            sends.append(d)
        return out_list

    def z_phase(part, dbuf, ybuf, zbuf, s, r, y_list):
        out_list = []
        for i in range(R):
            zt = zts[i]
            y_list[i].wait_recv()

            def add_body(j, carry, zt=zt):
                part[c, zt, y, j] = part[c, zt, y, j] + dbuf[zt, y, j] + ybuf[zt, j]
                return carry

            lax.fori_loop(0, hp, add_body, 0)
            if i < R - 1:
                d = rc(part.at[c, zt, y], zbuf.at[i], s.at[i], r.at[i], z_peer(zt), lay)
                d.start()
                out_list.append(d)
                sends.append(d)
        return out_list

    g_y = y_phase(gp, gd, gy, gy_s, gy_r, g_d)
    g_z = z_phase(gp, gd, gy, gz, gz_s, gz_r, g_y)

    for d in g_z:
        d.wait_recv()

    eye = (
        lax.broadcasted_iota(jnp.int32, (D, D), 0) == lax.broadcasted_iota(jnp.int32, (D, D), 1)
    ).astype(jnp.float32)
    scales = []
    for j in range(hp):
        total = gp[c, z, y, j]
        for i in range(R - 1):
            total = total + gz[i, j]
        mean = total[D:, :] / token_total
        slab[0, j, D:, :] = mean
        cov = total[:D, :] / token_total - dot_tt(mean, mean, HI) * (1.0 / PAD) + ridge_weight * eye
        norm2 = jnp.sum(jnp.sum(cov * cov, axis=1, keepdims=True), axis=0, keepdims=True)
        scale = jnp.sqrt(norm2)
        scales.append(scale)
        y0 = cov / scale
        f = 1.5 * eye - 0.5 * y0
        yb[j] = mm(y0, f)
        zb[j] = f

    def ns_body(t, carry):
        fs = [1.5 * eye - 0.5 * mm(zb[j], yb[j]) for j in range(hp)]
        for j in range(hp):
            yb[j] = mm(yb[j], fs[j])
            zb[j] = mm(fs[j], zb[j])
        return carry

    lax.fori_loop(1, ITERS - 1, ns_body, 0)
    for j in range(hp):
        f = 1.5 * eye - 0.5 * mm(zb[j], yb[j])
        w = mm(f, zb[j]) / jnp.sqrt(scales[j])
        slab[0, j, :D, :] = w
        wbuf[c, z, y, j] = w

    to_core = rc(slab.at[0], slab.at[1], p_s.at[0], p_r.at[0], core_peer, lay)
    to_lay = rc(slab.at[0], slab.at[2], q_s.at[0], q_r.at[0], me, other)
    to_core.start()
    to_lay.start()
    sends += [to_core, to_lay]

    a_z = []
    for i in range(R - 1):
        w_own = wbuf.at[c, z, y]
        d = rc(w_own, w_own, az_s.at[i], az_r.at[i], z_peer(zts[i]), lay)
        d.start()
        a_z.append(d)
        sends.append(d)

    def forward(e, zs):
        block = wbuf.at[c, zs, y]
        d = rc(block, block, ay_s.at[e], ay_r.at[e], y_peer, lay)
        d.start()
        f = rc(block, block, ad_s.at[2 * e], ad_r.at[2 * e], core_peer, lay)
        f.start()
        sends.extend([d, f])
        return d, f

    zss = [z] + [lax.rem(z + R - 1 - i, R) for i in range(R - 1)]
    a_y, a_d = [], []
    d, f = forward(0, z)
    a_y.append(d)
    a_d.append(f)

    c_d = []
    for i in range(R):
        zt = zts[i]
        if i < len(x_parts):
            x_parts[i].wait_recv()

        def cross_body(j, carry, zt=zt):
            for yy in range(2):
                cols = head_cols(zt, yy, j)
                v = x1[:, cols]
                cp[0, zt, yy, j] = dot_tt(v, x2[:, cols])
                cp[1, zt, yy, j] = dot_tt(v, x2o[:, cols])
            return carry

        lax.fori_loop(0, hp, cross_body, 0)
        d = rc(cp.at[1 - c, zt], cd.at[zt], cd_s.at[i], cd_r.at[i], core_peer, lay)
        d.start()
        c_d.append(d)
        sends.append(d)

    c_y = y_phase(cp, cd, cy, cy_s, cy_r, c_d)

    for i in range(R - 1):
        a_z[i].wait_recv()
        d, f = forward(i + 1, zss[i + 1])
        a_y.append(d)
        a_d.append(f)

    c_z = z_phase(cp, cd, cy, cz, cz_s, cz_r, c_y)

    for e in range(R):
        a_y[e].wait_recv()
        block = wbuf.at[c, zss[e], 1 - y]
        f = rc(block, block, ad_s.at[2 * e + 1], ad_r.at[2 * e + 1], core_peer, lay)
        f.start()
        a_d.append(f)
        sends.append(f)
    o1 = pltpu.make_async_copy(wbuf.at[c], out.at[c], o_s.at[0])
    o1.start()

    for d in c_z:
        d.wait_recv()
    to_core.wait_recv()
    to_lay.wait_recv()
    sub = lax.broadcasted_iota(jnp.int32, sbuf.shape[1:], 0)
    tile = jnp.zeros(sbuf.shape[1:], jnp.float32)
    for j in range(hp):
        total = cp[c, z, y, j]
        for i in range(R - 1):
            total = total + cz[i, j]
        left = slab[c, j]
        right = slab[1 + c, j]
        cross = total / token_total - dot_tt(left[D:, :], right[D:, :], HI) * (1.0 / PAD)
        white = mm(mm(left[:D, :], cross), right[:D, :])
        value = jnp.sum(jnp.sum(white * white, axis=1, keepdims=True), axis=0, keepdims=True) / HEAD_DIM
        tile = jnp.where(sub == j, value, tile)
    sbuf[me] = tile
    s_list = []
    for k in range(1, n):
        d = rc(sbuf.at[me], sbuf.at[me], ss_s.at[k], ss_r.at[k], lax.rem(me + k, n), lay)
        d.start()
        s_list.append(d)
        sends.append(d)

    for f in a_d:
        f.wait_recv()
    o2 = pltpu.make_async_copy(wbuf.at[1 - c], out.at[1 - c], o_s.at[1])
    o2.start()
    for d in s_list:
        d.wait_recv()
    simout[...] = sbuf[...]
    o1.wait()
    o2.wait()
    for d in sends:
        d.wait_send()


def solution(mesh):
    n = mesh.shape["tok"]
    R = n // 4
    hp = -(-HEADS // (n // 2))
    srows = -(-hp // 8) * 8
    D = HEAD_DIM
    E = D + PAD

    def local(first_acts, second_acts):
        _, rows, width = first_acts.shape
        token_total = float(rows * n)
        f32 = jnp.float32
        dma = lambda k: pltpu.SemaphoreType.DMA((max(k, 1),))
        out, sims = pl.pallas_call(
            functools.partial(kernel, n, R, hp, token_total),
            out_shape=(
                jax.ShapeDtypeStruct((2, R, 2, hp, D, D), f32),
                jax.ShapeDtypeStruct((n, srows, D), f32),
            ),
            in_specs=[pl.BlockSpec(memory_space=pltpu.VMEM)] * 2,
            out_specs=(
                pl.BlockSpec(memory_space=pltpu.MemorySpace.HBM),
                pl.BlockSpec(memory_space=pltpu.VMEM),
            ),
            scratch_shapes=[
                pltpu.VMEM((rows, width), jnp.bfloat16),
                pltpu.VMEM((2, R, 2, hp, E, D), f32),
                pltpu.VMEM((R, 2, hp, E, D), f32),
                pltpu.VMEM((R, hp, E, D), f32),
                pltpu.VMEM((R - 1, hp, E, D), f32),
                pltpu.VMEM((2, R, 2, hp, D, D), f32),
                pltpu.VMEM((R, 2, hp, D, D), f32),
                pltpu.VMEM((R, hp, D, D), f32),
                pltpu.VMEM((R - 1, hp, D, D), f32),
                pltpu.VMEM((3, hp, E, D), f32),
                pltpu.VMEM((2, R, 2, hp, D, D), f32),
                pltpu.VMEM((n, srows, D), f32),
                pltpu.VMEM((hp, D, D), f32),
                pltpu.VMEM((hp, D, D), f32),
                dma(R), dma(R),
                dma(R), dma(R), dma(R), dma(R), dma(R - 1), dma(R - 1),
                dma(R), dma(R), dma(R), dma(R), dma(R - 1), dma(R - 1),
                dma(1), dma(1), dma(1), dma(1),
                dma(R - 1), dma(R - 1), dma(R), dma(R), dma(2 * R), dma(2 * R),
                dma(n), dma(n),
                dma(2),
            ],
            compiler_params=pltpu.CompilerParams(
                collective_id=0, has_side_effects=True, vmem_limit_bytes=58 * 1024 * 1024
            ),
        )(first_acts[0], second_acts[0])
        whitening = out.reshape(2, R * 2 * hp, D, D)[:, None, :HEADS]
        s = sims[:, :hp, 0].reshape(R * 2, 2, hp).transpose(1, 0, 2).reshape(2, R * 2 * hp)[:, :HEADS]
        s = jnp.where(lax.axis_index("lay") == 0, s, s[::-1])
        return whitening, s[None]

    in_specs = (P("lay", "tok", None), P("lay", "tok", None))
    out_specs = (P(None, "lay", None, None, None), P("lay", None, None))
    return jax.shard_map(local, mesh=mesh, in_specs=in_specs, out_specs=out_specs, check_vma=False)
```

```python
import functools

import jax
import jax.numpy as jnp
from jax import lax
from jax.experimental import pallas as pl
from jax.experimental.pallas import tpu as pltpu
from jax.sharding import PartitionSpec as P

HEADS = 40
HEAD_DIM = 128
ITERS = 6
PAD = 8

ridge_weight = 0.05
MESH = pl.DeviceIdType.MESH
HI = lax.Precision.HIGHEST


def dot_tt(a, b, precision=None):
    return lax.dot_general(
        a, b, (((0,), (0,)), ((), ())), preferred_element_type=jnp.float32, precision=precision
    )


def mm(a, b):
    return jnp.dot(a, b, preferred_element_type=jnp.float32, precision=HI)


BLOCKS = HEAD_DIM // 8
KEPT = BLOCKS // 2 + 1
PACKED = 8 * KEPT


def lane_block():
    return lax.broadcasted_iota(jnp.int32, (8, HEAD_DIM), 1) // 8


def pack(a):
    lb = lane_block()
    xs = [a[8 * e : 8 * e + 8, :] for e in range(BLOCKS)]
    step = 1
    while step < BLOCKS:
        bit = (lb // step) % 2 == 1
        xs = [jnp.where(bit, xs[(e + step) % BLOCKS], xs[e]) for e in range(BLOCKS)]
        step *= 2
    return jnp.concatenate([xs[(-d) % BLOCKS] for d in range(KEPT)], axis=0)


def unpack(p):
    lb = lane_block()
    zero = jnp.zeros((8, HEAD_DIM), jnp.float32)
    ys = [zero] * BLOCKS
    for d in range(KEPT):
        ys[(-d) % BLOCKS] = p[8 * d : 8 * d + 8, :]
    step = 1
    while step < BLOCKS:
        bit = (lb // step) % 2 == 1
        ys = [jnp.where(bit, ys[(e - step) % BLOCKS], ys[e]) for e in range(BLOCKS)]
        step *= 2
    half = jnp.concatenate(ys, axis=0)
    rb = lax.broadcasted_iota(jnp.int32, (HEAD_DIM, HEAD_DIM), 0) // 8
    cb = lax.broadcasted_iota(jnp.int32, (HEAD_DIM, HEAD_DIM), 1) // 8
    return jnp.where((cb - rb + BLOCKS) % BLOCKS < KEPT, half, half.T)


def kernel(
    n, R, hp, token_total,
    x1, x2, out, simout,
    x2o, gp, gd, gy, gz, cp, cd, cys, cy, czs, cz, slab, wbuf, wfull, sbuf, yb, zb,
    x_s, x_r, gd_s, gd_r, gy_s, gy_r, gz_s, gz_r,
    cd_s, cd_r, cy_s, cy_r, cz_s, cz_r,
    p_s, p_r, q_s, q_r, az_s, az_r, ay_s, ay_r, ad_s, ad_r, ss_s, ss_r, o_s,
):
    me = lax.axis_index("tok")
    lay = lax.axis_index("lay")
    other = 1 - lay
    c = lax.rem(me, 2)
    y = lax.rem(me // 2, 2)
    z = me // 4
    rows = x1.shape[0]
    D = HEAD_DIM
    core_peer = z * 4 + y * 2 + (1 - c)
    y_peer = z * 4 + (1 - y) * 2 + c

    def z_peer(zt):
        return zt * 4 + y * 2 + c

    def rc(src, dst, s, r, tok, ly):
        return pltpu.make_async_remote_copy(
            src_ref=src, dst_ref=dst, send_sem=s, recv_sem=r,
            device_id=(tok, ly), device_id_type=MESH,
        )

    barrier = pltpu.get_barrier_semaphore()
    for k in range(1, n):
        pl.semaphore_signal(barrier, inc=1, device_id=(lax.rem(me + k, n), lay), device_id_type=MESH)
    pl.semaphore_signal(barrier, inc=1, device_id=(me, other), device_id_type=MESH)
    pl.semaphore_wait(barrier, n)

    zts = [lax.rem(z + 1 + i, R) for i in range(R)]
    sends = []

    padded = R * 2 * hp != HEADS
    width = x1.shape[1] // R if not padded else x1.shape[1]
    x_parts = []
    for i in range(R if not padded else 1):
        cols = pl.ds(pl.multiple_of(zts[i] * width, 128), width) if not padded else pl.ds(0, width)
        d = rc(x2.at[:, cols], x2o.at[:, cols], x_s.at[i], x_r.at[i], me, other)
        d.start()
        x_parts.append(d)
        sends.append(d)

    def head_cols(zt, yy, j):
        h = (zt * 2 + yy) * hp + j
        if padded:
            h = jnp.minimum(h, HEADS - 1)
        return pl.ds(pl.multiple_of(h * D, D), D)

    ones = jnp.ones((PAD, rows), jnp.bfloat16)

    g_d = []
    for i in range(R):
        zt = zts[i]

        def gram_body(j, carry, zt=zt):
            for yy in range(2):
                cols = head_cols(zt, yy, j)
                for k, ref in enumerate((x1, x2)):
                    v = ref[:, cols]
                    gp[k, zt, yy, j, :PACKED, :] = pack(dot_tt(v, v))
                    gp[k, zt, yy, j, PACKED:, :] = jnp.dot(ones, v, preferred_element_type=jnp.float32)
            return carry

        lax.fori_loop(0, hp, gram_body, 0)
        d = rc(gp.at[1 - c, zt], gd.at[zt], gd_s.at[i], gd_r.at[i], core_peer, lay)
        d.start()
        g_d.append(d)
        sends.append(d)

    def y_phase(part, dbuf, ybuf, s, r, d_list):
        out_list = []
        for i in range(R):
            zt = zts[i]
            d_list[i].wait_recv()

            def add_body(j, carry, zt=zt):
                part[c, zt, 1 - y, j] = part[c, zt, 1 - y, j] + dbuf[zt, 1 - y, j]
                return carry

            lax.fori_loop(0, hp, add_body, 0)
            d = rc(part.at[c, zt, 1 - y], ybuf.at[zt], s.at[i], r.at[i], y_peer, lay)
            d.start()
            out_list.append(d)
            sends.append(d)
        return out_list

    def z_phase(part, dbuf, ybuf, zbuf, s, r, y_list):
        out_list = []
        for i in range(R):
            zt = zts[i]
            y_list[i].wait_recv()

            def add_body(j, carry, zt=zt):
                part[c, zt, y, j] = part[c, zt, y, j] + dbuf[zt, y, j] + ybuf[zt, j]
                return carry

            lax.fori_loop(0, hp, add_body, 0)
            if i < R - 1:
                d = rc(part.at[c, zt, y], zbuf.at[i], s.at[i], r.at[i], z_peer(zt), lay)
                d.start()
                out_list.append(d)
                sends.append(d)
        return out_list

    g_y = y_phase(gp, gd, gy, gy_s, gy_r, g_d)

    def c_d(i):
        return rc(cp.at[1 - c, zts[i]], cd.at[zts[i]], cd_s.at[i], cd_r.at[i], core_peer, lay)

    def c_y(i):
        return rc(cys.at[zts[i]], cy.at[zts[i]], cy_s.at[i], cy_r.at[i], y_peer, lay)

    def c_z(i):
        return rc(czs.at[zts[i]], cz.at[i], cz_s.at[i], cz_r.at[i], z_peer(zts[i]), lay)

    def cross_chunk(k, ref, i):
        zt = zts[i]

        def body(j, carry):
            for yy in range(2):
                cols = head_cols(zt, yy, j)
                cp[k, zt, yy, j] = dot_tt(x1[:, cols], ref[:, cols])
            return carry

        lax.fori_loop(0, hp, body, 0)

        @pl.when(c == 1 - k)
        def _():
            c_d(i).start()

    def cross_y(k):
        @pl.when(c == k)
        def _():
            for i in range(R):
                zt = zts[i]
                c_d(i).wait_recv()

                def body(j, carry, zt=zt):
                    total = cp[k, zt, 1 - y, j] + cd[zt, 1 - y, j]
                    cys[zt, j] = total
                    return carry

                lax.fori_loop(0, hp, body, 0)
                c_y(i).start()

    def cross_z(k):
        @pl.when(c == k)
        def _():
            for i in range(R):
                zt = zts[i]
                c_y(i).wait_recv()

                def body(j, carry, zt=zt, last=i == R - 1):
                    total = cp[k, zt, y, j] + cd[zt, y, j] + cy[zt, j]
                    if last:
                        cp[k, zt, y, j] = total
                    else:
                        czs[zt, j] = total
                    return carry

                lax.fori_loop(0, hp, body, 0)
                if i < R - 1:
                    c_z(i).start()

    for i in range(R):
        cross_chunk(0, x2, i)
    g_z = z_phase(gp, gd, gy, gz, gz_s, gz_r, g_y)
    cross_y(0)

    for d in g_z:
        d.wait_recv()

    eye = (
        lax.broadcasted_iota(jnp.int32, (D, D), 0) == lax.broadcasted_iota(jnp.int32, (D, D), 1)
    ).astype(jnp.float32)
    scales = []
    for j in range(hp):
        total = gp[c, z, y, j]
        for i in range(R - 1):
            total = total + gz[i, j]
        mean = total[PACKED:, :] / token_total
        slab[0, j, D:, :] = mean
        cov = unpack(total[:PACKED, :]) / token_total - dot_tt(mean, mean, HI) * (1.0 / PAD) + ridge_weight * eye
        norm2 = jnp.sum(jnp.sum(cov * cov, axis=1, keepdims=True), axis=0, keepdims=True)
        scale = jnp.sqrt(norm2)
        scales.append(scale)
        y0 = cov / scale
        f = 1.5 * eye - 0.5 * y0
        yb[j] = mm(y0, f)
        zb[j] = f

    def ns_body(t, carry):
        fs = [1.5 * eye - 0.5 * mm(zb[j], yb[j]) for j in range(hp)]
        for j in range(hp):
            yb[j] = mm(yb[j], fs[j])
            zb[j] = mm(fs[j], zb[j])
        return carry

    lax.fori_loop(1, ITERS - 1, ns_body, 0)
    for j in range(hp):
        f = 1.5 * eye - 0.5 * mm(zb[j], yb[j])
        w = mm(f, zb[j]) / jnp.sqrt(scales[j])
        slab[0, j, :D, :] = w
        wbuf[c, z, y, j] = pack(w)
        wfull[c, z, y, j] = w

    to_core = rc(slab.at[0], slab.at[1], p_s.at[0], p_r.at[0], core_peer, lay)
    to_lay = rc(slab.at[0], slab.at[2], q_s.at[0], q_r.at[0], me, other)
    to_core.start()
    to_lay.start()
    sends += [to_core, to_lay]

    a_z = []
    for i in range(R - 1):
        w_own = wbuf.at[c, z, y]
        d = rc(w_own, w_own, az_s.at[i], az_r.at[i], z_peer(zts[i]), lay)
        d.start()
        a_z.append(d)
        sends.append(d)

    def forward(e, zs):
        block = wbuf.at[c, zs, y]
        d = rc(block, block, ay_s.at[e], ay_r.at[e], y_peer, lay)
        d.start()
        f = rc(block, block, ad_s.at[2 * e], ad_r.at[2 * e], core_peer, lay)
        f.start()
        sends.extend([d, f])
        return d, f

    zss = [z] + [lax.rem(z + R - 1 - i, R) for i in range(R - 1)]
    a_y, a_d = [], []
    d, f = forward(0, z)
    a_y.append(d)
    a_d.append(f)

    outs = []

    def emit(cc, zs, yy):
        d = pltpu.make_async_copy(wfull.at[cc, zs, yy], out.at[cc, zs, yy], o_s.at[len(outs)])
        d.start()
        outs.append(d)

    def expand(cc, zs, yy):
        def body(j, carry):
            wfull[cc, zs, yy, j] = unpack(wbuf[cc, zs, yy, j])
            return carry

        lax.fori_loop(0, hp, body, 0)
        emit(cc, zs, yy)

    emit(c, z, y)
    cross_z(0)

    for i in range(R):
        if i < len(x_parts):
            x_parts[i].wait_recv()
        cross_chunk(1, x2o, i)
    cross_y(1)

    for i in range(R - 1):
        a_z[i].wait_recv()
        d, f = forward(i + 1, zss[i + 1])
        a_y.append(d)
        a_d.append(f)

    cross_z(1)

    for e in range(1, R):
        expand(c, zss[e], y)
    for e in range(R):
        a_y[e].wait_recv()
        block = wbuf.at[c, zss[e], 1 - y]
        f = rc(block, block, ad_s.at[2 * e + 1], ad_r.at[2 * e + 1], core_peer, lay)
        f.start()
        a_d.append(f)
        sends.append(f)
        expand(c, zss[e], 1 - y)

    for i in range(R - 1):
        c_z(i).wait_recv()
    to_core.wait_recv()
    to_lay.wait_recv()
    sub = lax.broadcasted_iota(jnp.int32, sbuf.shape[1:], 0)
    tile = jnp.zeros(sbuf.shape[1:], jnp.float32)
    for j in range(hp):
        total = cp[c, z, y, j]
        for i in range(R - 1):
            total = total + cz[i, j]
        left = slab[c, j]
        right = slab[1 + c, j]
        cross = total / token_total - dot_tt(left[D:, :], right[D:, :], HI) * (1.0 / PAD)
        white = mm(mm(left[:D, :], cross), right[:D, :])
        value = jnp.sum(jnp.sum(white * white, axis=1, keepdims=True), axis=0, keepdims=True) / HEAD_DIM
        tile = jnp.where(sub == j, value, tile)
    sbuf[me] = tile
    s_list = []
    for k in range(1, n):
        d = rc(sbuf.at[me], sbuf.at[me], ss_s.at[k], ss_r.at[k], lax.rem(me + k, n), lay)
        d.start()
        s_list.append(d)
        sends.append(d)

    for e in range(R):
        a_d[e].wait_recv()
        expand(1 - c, zss[e], y)
    for e in range(R):
        a_d[R + e].wait_recv()
        expand(1 - c, zss[e], 1 - y)
    for d in s_list:
        d.wait_recv()
    simout[...] = sbuf[...]
    for d in outs:
        d.wait()
    for d in sends:
        d.wait_send()
    for i in range(R):
        c_d(i).wait_send()
        c_y(i).wait_send()
    for i in range(R - 1):
        c_z(i).wait_send()


def solution(mesh):
    n = mesh.shape["tok"]
    R = n // 4
    hp = -(-HEADS // (n // 2))
    srows = -(-hp // 8) * 8
    D = HEAD_DIM
    E = PACKED + PAD

    def local(first_acts, second_acts):
        _, rows, width = first_acts.shape
        token_total = float(rows * n)
        f32 = jnp.float32
        dma = lambda k: pltpu.SemaphoreType.DMA((max(k, 1),))
        out, sims = pl.pallas_call(
            functools.partial(kernel, n, R, hp, token_total),
            out_shape=(
                jax.ShapeDtypeStruct((2, R, 2, hp, D, D), f32),
                jax.ShapeDtypeStruct((n, srows, D), f32),
            ),
            in_specs=[pl.BlockSpec(memory_space=pltpu.VMEM)] * 2,
            out_specs=(
                pl.BlockSpec(memory_space=pltpu.MemorySpace.HBM),
                pl.BlockSpec(memory_space=pltpu.VMEM),
            ),
            scratch_shapes=[
                pltpu.VMEM((rows, width), jnp.bfloat16),
                pltpu.VMEM((2, R, 2, hp, E, D), f32),
                pltpu.VMEM((R, 2, hp, E, D), f32),
                pltpu.VMEM((R, hp, E, D), f32),
                pltpu.VMEM((R - 1, hp, E, D), f32),
                pltpu.VMEM((2, R, 2, hp, D, D), f32),
                pltpu.VMEM((R, 2, hp, D, D), f32),
                pltpu.VMEM((R, hp, D, D), f32),
                pltpu.VMEM((R, hp, D, D), f32),
                pltpu.VMEM((R, hp, D, D), f32),
                pltpu.VMEM((R - 1, hp, D, D), f32),
                pltpu.VMEM((3, hp, D + PAD, D), f32),
                pltpu.VMEM((2, R, 2, hp, PACKED, D), f32),
                pltpu.VMEM((2, R, 2, hp, D, D), f32),
                pltpu.VMEM((n, srows, D), f32),
                pltpu.VMEM((hp, D, D), f32),
                pltpu.VMEM((hp, D, D), f32),
                dma(R), dma(R),
                dma(R), dma(R), dma(R), dma(R), dma(R - 1), dma(R - 1),
                dma(R), dma(R), dma(R), dma(R), dma(R - 1), dma(R - 1),
                dma(1), dma(1), dma(1), dma(1),
                dma(R - 1), dma(R - 1), dma(R), dma(R), dma(2 * R), dma(2 * R),
                dma(n), dma(n),
                dma(4 * R),
            ],
            compiler_params=pltpu.CompilerParams(
                collective_id=0, has_side_effects=True, vmem_limit_bytes=58 * 1024 * 1024
            ),
        )(first_acts[0], second_acts[0])
        whitening = out.reshape(2, R * 2 * hp, D, D)[:, None, :HEADS]
        s = sims[:, :hp, 0].reshape(R * 2, 2, hp).transpose(1, 0, 2).reshape(2, R * 2 * hp)[:, :HEADS]
        s = jnp.where(lax.axis_index("lay") == 0, s, s[::-1])
        return whitening, s[None]

    in_specs = (P("lay", "tok", None), P("lay", "tok", None))
    out_specs = (P(None, "lay", None, None, None), P("lay", None, None))
    return jax.shard_map(local, mesh=mesh, in_specs=in_specs, out_specs=out_specs, check_vma=False)
```
